32 devices in a mesh: date: 4 (over y, x), pix: 8 (over z, core).
Axes of the slice: x: 2, y: 2, z: 4, core: 2. Of those that a mesh axis runs over, the one named last changes fastest.
Arguments:
- stack: bfloat16 [64, 7, 64, 1024], P('date', None, None, 'pix'), may hold values from -8 to 8
- quality: int32 [64, 64, 1024], P('date', None, 'pix'), may hold values from 0 to 1073741823
- days: int32 [64], P('date'), may hold values from 8 to 1536, as said below
Outputs:
- coef: float32 [7, 8, 64, 1024], P(None, None, 'pix', 'date')
- score: float32 [7, 64, 1024], P(None, 'pix', 'date')
The draws below stay inside these ranges and needn't reach their ends.
Inputs may be any that keep to these rules, and one draw needn't show every extreme that they name: `days`: strictly increasing.
All inputs are finite; a program needn't handle non-finite values.
Results may differ from the reference program's by a relative error of at most 0.0003.
Values may be sent and summed in bfloat16 or wider, within the bound.
A program may use at most 256 MiB of HBM per device.

```python
import jax
import jax.numpy as jnp
from jax import lax

DATES = 64
BANDS = 7
HARM = 8
ROWS = 64
COLS = 1024


def make_days(key):
    inner_count = 24 * DATES - 9
    order = jax.random.permutation(jax.random.fold_in(key, 11), inner_count)
    chosen = jnp.sort(order[:DATES - 2]).astype(jnp.int32) + 9
    first = jnp.full((1,), 8, dtype=jnp.int32)
    last = jnp.full((1,), 24 * DATES, dtype=jnp.int32)
    return jnp.concatenate([first, chosen, last]).astype(jnp.int32)


def design_matrix_drawn(days):
    moment_t = days.astype(jnp.float32)
    columns = [jnp.ones_like(moment_t), (moment_t - 512.0) / 512.0]
    for order in range(1, 4):
        phase = 2.0 * jnp.pi * order * moment_t / 365.25
        columns.append(jnp.cos(phase))
        columns.append(jnp.sin(phase))
    return jnp.stack(columns, 1)


def draw_days(key, part):
    return make_days(key)


def draw_quality(key, part):
    shape = (DATES, ROWS, COLS)
    bits = jax.random.randint(jax.random.fold_in(key, 21), shape, 0, 2 ** 30)
    rows = jnp.arange(ROWS, dtype=jnp.int32)
    cols = jnp.arange(COLS, dtype=jnp.int32)
    row_limit = 300 * rows // max(ROWS - 1, 1)
    col_limit = 300 * cols // max(COLS - 1, 1)
    limit = 200 + row_limit[:, None] + col_limit[None, :]
    rolled = jax.random.randint(jax.random.fold_in(key, 22), shape, 0, 1000)
    cloud = (rolled < limit[None, :, :]).astype(jnp.int32)
    return (bits - jnp.bitwise_and(bits, 8) + 8 * cloud).astype(jnp.int32)


def draw_stack(key, part):
    design = design_matrix_drawn(make_days(key))
    coefs = 0.6 * jax.random.normal(jax.random.fold_in(key, 31), (HARM, BANDS, ROWS, COLS), jnp.float32)
    rough = jax.random.uniform(jax.random.fold_in(key, 32), (BANDS, ROWS, COLS), jnp.float32, 0.5, 1.5)
    rows = jnp.arange(ROWS, dtype=jnp.float32)
    cols = jnp.arange(COLS, dtype=jnp.float32)
    row_scale = 0.15 * jnp.power(3.2, rows / max(ROWS - 1, 1))
    col_scale = jnp.power(3.2, cols / max(COLS - 1, 1))
    scale_map = row_scale[:, None] * col_scale[None, :]
    shape = (DATES, BANDS, ROWS, COLS)
    noise = jax.random.normal(jax.random.fold_in(key, 33), shape, jnp.float32)
    signal = jnp.einsum('tk,kbrc->tbrc', design, coefs)
    values = signal + noise * rough[None] * scale_map[None, None, :, :]
    return jnp.clip(values, -8.0, 8.0).astype(jnp.bfloat16)


def setup_inputs(seed: int = 0) -> dict:
    key_of = jax.random.split(jax.random.key(seed), 4)
    stack = draw_stack(jax.random.fold_in(key_of[3], 71), 0)
    quality = draw_quality(jax.random.fold_in(key_of[3], 71), 0)
    days = draw_days(jax.random.fold_in(key_of[3], 71), 0)
    return {"stack": stack, "quality": quality, "days": days}


RIDGE_TERM = 1.0
PAIR_LIST = [(first, second) for first in range(8) for second in range(first, 8)]

def design_matrix(days):
    moment_t = days.astype(jnp.float32)
    columns = [jnp.ones_like(moment_t), (moment_t - 512.0) / 512.0]
    for order in range(1, 4):
        phase = 2.0 * jnp.pi * order * moment_t / 365.25
        columns.append(jnp.cos(phase))
        columns.append(jnp.sin(phase))
    return jnp.stack(columns, 1)

def weights(quality):
    cloud = jnp.bitwise_and(jnp.right_shift(quality, 3), 1)
    level = jnp.bitwise_and(jnp.right_shift(quality, 8), 3)
    return (1 - cloud).astype(jnp.float32) / (1.0 + level.astype(jnp.float32))

def reference(stack, quality, days):
    design = design_matrix(days)
    products = jnp.stack([design[:, first] * design[:, second] for first, second in PAIR_LIST], 1)
    index_table = [[0] * 8 for first in range(8)]
    for number, pair in enumerate(PAIR_LIST):
        index_table[pair[0]][pair[1]] = number
        index_table[pair[1]][pair[0]] = number
    index_array = jnp.array(index_table, dtype=jnp.int32)
    high = lax.Precision.HIGHEST

    def row_fit(row):
        values = lax.dynamic_slice_in_dim(stack, row, 1, 2)[:, :, 0, :].astype(jnp.float32)
        bits = lax.dynamic_slice_in_dim(quality, row, 1, 1)[:, 0, :]
        weight = weights(bits)
        gram = jnp.dot(products.T, weight, precision=high)
        moment = jnp.einsum('tk,tbc->kbc', design, weight[:, None, :] * values, precision=high)
        full = jnp.transpose(gram[index_array], (2, 0, 1)) + RIDGE_TERM * jnp.eye(8, dtype=jnp.float32)
        solved = jnp.linalg.solve(full, jnp.transpose(moment, (2, 0, 1)))
        coef_row = jnp.transpose(solved, (1, 2, 0))
        fitted = jnp.einsum('tk,kbc->tbc', design, coef_row, precision=high)
        ssr = lax.optimization_barrier(jnp.sum(weight[:, None, :] * (values - fitted) ** 2, 0))
        return (coef_row, ssr, lax.optimization_barrier(jnp.sum(weight, 0)))
    coef_rows, ssr, wsum = lax.map(row_fit, jnp.arange(ROWS, dtype=jnp.int32))
    sigma2 = lax.optimization_barrier(jnp.sum(ssr, (0, 2))) / jnp.sum(wsum)
    score = jnp.sqrt(ssr / (wsum[:, None, :] + 1.0)) / jnp.sqrt(sigma2)[None, :, None]
    return (jnp.transpose(coef_rows, (2, 1, 0, 3)), jnp.transpose(score, (1, 0, 2)))
```

```python
import functools

import jax
import jax.numpy as jnp
from jax import lax
from jax.experimental import pallas as pl
from jax.experimental.pallas import tpu as pltpu
from jax.sharding import PartitionSpec as P

RIDGE_TERM = 1.0
HARM = 8
LAG = 2
MESH = pl.DeviceIdType.MESH
PAIR_LIST = [(first, second) for first in range(HARM) for second in range(first + 1)]
PAIR_AT = {pair: number for number, pair in enumerate(PAIR_LIST)}


def design_matrix(days):
    moment_t = days.astype(jnp.float32)
    columns = [jnp.ones_like(moment_t), (moment_t - 512.0) / 512.0]
    for order in range(1, 4):
        phase = 2.0 * jnp.pi * order * moment_t / 365.25
        columns.append(jnp.cos(phase))
        columns.append(jnp.sin(phase))
    return jnp.stack(columns, 1)


def kernel(dims, stack, quality, des_in, coef, score,
           qbuf, code, raw, dall, bdes, wbuf, lbuf, wsum_ref, res, rel, fin,
           ssum, part, part_date, part_mid, part_pix,
           q_sem, des_send, des_recv, raw_send, raw_recv,
           hop_send, rel_recv, fin_send, fin_recv,
           pd_send, pd_recv, pp_send, pp_recv):
    dates, pixes, times, bands, block = dims
    per = pixes // dates
    s = lax.axis_index("date")
    q = lax.axis_index("pix")
    total = dates * times
    home = q // per

    def target(sd, j):
        return per * lax.rem(sd + per * lax.rem(q, 2) + j, dates) + j

    def owner(qq, p):
        shift = per * lax.rem(qq, 2) + lax.rem(p, per)
        return lax.rem(p // per + 64 * dates - shift, dates)

    barrier = pltpu.get_barrier_semaphore()
    for k in range(1, dates):
        pl.semaphore_signal(barrier, inc=1, device_id=(lax.rem(s + k, dates), q),
                            device_id_type=MESH)
    for k in range(1, pixes):
        pl.semaphore_signal(barrier, inc=1, device_id=(s, lax.rem(q + k, pixes)),
                            device_id_type=MESH)

    q_copy = pltpu.make_async_copy(quality, qbuf, q_sem)
    q_copy.start()

    def own_copy(j, b):
        rows = pl.ds(pl.multiple_of(target(s, j) * block, block), block)
        return pltpu.make_async_copy(
            stack.at[:, b, rows, :], raw.at[j, b, pl.ds(s * times, times)],
            raw_recv.at[j, b, s])

    def own_code(j):
        return pltpu.make_async_copy(
            code.at[target(s, j)], raw.at[j, bands, pl.ds(s * times, times)],
            raw_recv.at[j, bands, s])

    for j in range(per):
        for b in range(bands):
            own_copy(j, b).start()

    q_copy.wait()
    for p in range(pixes):
        bits = qbuf[:, p * block:(p + 1) * block, :]
        cloud = jnp.bitwise_and(jnp.right_shift(bits, 3), 1)
        level = jnp.bitwise_and(jnp.right_shift(bits, 8), 3)
        code[p] = ((1 - cloud) * (1 + level)).astype(jnp.float32).astype(jnp.bfloat16)

    pl.semaphore_wait(barrier, dates - 1 + pixes - 1)

    def des_copy(k):
        return pltpu.make_async_remote_copy(
            des_in, dall.at[s], des_send.at[k], des_recv.at[s],
            device_id=(lax.rem(s + k, dates), q), device_id_type=MESH)

    def raw_copy(j, b, k):
        peer = lax.rem(s + k, dates)
        rows = pl.ds(pl.multiple_of(target(peer, j) * block, block), block)
        return pltpu.make_async_remote_copy(
            stack.at[:, b, rows, :], raw.at[j, b, pl.ds(s * times, times)],
            raw_send.at[j, b, k], raw_recv.at[j, b, s],
            device_id=(peer, q), device_id_type=MESH)

    def code_copy(j, k):
        peer = lax.rem(s + k, dates)
        return pltpu.make_async_remote_copy(
            code.at[target(peer, j)], raw.at[j, bands, pl.ds(s * times, times)],
            raw_send.at[j, bands, k], raw_recv.at[j, bands, s],
            device_id=(peer, q), device_id_type=MESH)

    for k in range(1, dates):
        des_copy(k).start()
    for j in range(per):
        own_code(j).start()
        for k in range(1, dates):
            code_copy(j, k).start()
    for j in range(per):
        for b in range(bands):
            for k in range(1, dates):
                raw_copy(j, b, k).start()

    def raw_wait(j, b, sd):
        pltpu.make_async_copy(
            raw.at[j, b, pl.ds(sd * times, times)],
            raw.at[j, b, pl.ds(sd * times, times)],
            raw_recv.at[j, b, sd]).wait()

    dall[s] = des_in[...]
    for k in range(1, dates):
        sd = lax.rem(s + k, dates)
        pltpu.make_async_copy(dall.at[sd], dall.at[sd], des_recv.at[sd]).wait()

    @pl.loop(0, total)
    def _(t):
        row = dall[t // times, pl.ds(lax.rem(t, times), 1), :]
        for i in range(HARM):
            bdes[t, i] = jnp.broadcast_to(row[:, i:i + 1], (block, 128))

    zero = jnp.zeros((block, 128), jnp.float32)
    for b in range(bands + 1):
        ssum[b] = zero

    def gram_step(j):
        for sd in range(dates):
            raw_wait(j, bands, sd)

        def body(t, carry):
            value = raw[j, bands, t].astype(jnp.float32)
            w = jnp.where(value == 0.0, 0.0, 1.0 / jnp.maximum(value, 1.0))
            wbuf[t] = w
            d = [bdes[t, i] for i in range(HARM)]
            wd = [w] + [w * d[i] for i in range(1, HARM)]
            return tuple(
                carry[n] + (wd[first] if second == 0 else wd[first] * d[second])
                for n, (first, second) in enumerate(PAIR_LIST))

        gram = lax.fori_loop(0, total, body, (zero,) * len(PAIR_LIST), unroll=2)
        wsum_ref[...] = gram[0]
        ssum[bands] = ssum[bands] + gram[0]
        lower = {}
        for first in range(HARM):
            for second in range(first + 1):
                value = gram[PAIR_AT[first, second]]
                if first == second:
                    value = value + RIDGE_TERM
                for inner in range(second):
                    value = value - lower[first, inner] * lower[second, inner]
                if first == second:
                    lower[first, first] = 1.0 / jnp.sqrt(value)
                else:
                    lower[first, second] = value * lower[second, second]
                lbuf[PAIR_AT[first, second]] = lower[first, second]

    def hop(j, b, start):
        p = target(s, j)

        def act(dst, sem):
            @pl.when(p != q)
            def _():
                c = pltpu.make_async_remote_copy(
                    res.at[j, b], dst, hop_send.at[j, b], sem,
                    device_id=(s, p), device_id_type=MESH)
                c.start() if start else c.wait_send()

            if start:
                @pl.when(p == q)
                def _():
                    pltpu.make_async_copy(res.at[j, b], dst, sem).start()

        @pl.when(home == s)
        def _():
            act(fin.at[lax.rem(q, per), b], fin_recv.at[lax.rem(q, per), b])

        @pl.when(home != s)
        def _():
            act(rel.at[q, b], rel_recv.at[q, b])

    def band_step(j, b):
        for sd in range(dates):
            raw_wait(j, b, sd)

        def body(t, carry):
            wy = wbuf[t] * raw[j, b, t].astype(jnp.float32)
            return tuple(
                carry[i] + (wy if i == 0 else bdes[t, i] * wy) for i in range(HARM))

        moment = lax.fori_loop(0, total, body, (zero,) * HARM, unroll=8)
        low = lambda first, second: lbuf[PAIR_AT[first, second]]
        forward = []
        for first in range(HARM):
            value = moment[first]
            for inner in range(first):
                value = value - low(first, inner) * forward[inner]
            forward.append(value * low(first, first))
        back = [None] * HARM
        for first in range(HARM - 1, -1, -1):
            value = forward[first]
            for inner in range(HARM - 1, first, -1):
                value = value - low(inner, first) * back[inner]
            back[first] = value * low(first, first)
        for i in range(HARM):
            res[j, b, i] = back[i]

        def residual(t, ssr):
            terms = [back[0]] + [bdes[t, i] * back[i] for i in range(1, HARM)]
            while len(terms) > 1:
                terms = [terms[i] + terms[i + 1] for i in range(0, len(terms), 2)]
            diff = raw[j, b, t].astype(jnp.float32) - terms[0]
            return ssr + wbuf[t] * diff * diff

        ssr = lax.fori_loop(0, total, residual, zero, unroll=8)
        res[j, b, HARM] = jnp.sqrt(ssr / (wsum_ref[...] + 1.0))
        ssum[b] = ssum[b] + ssr
        hop(j, b, True)

    def pass_on(qq, b, start):
        far = qq // per

        @pl.when(jnp.logical_and(owner(qq, q) == s, far != s))
        def _():
            c = pltpu.make_async_remote_copy(
                rel.at[qq, b], fin.at[lax.rem(qq, per), b], fin_send.at[qq, b],
                fin_recv.at[lax.rem(qq, per), b],
                device_id=(far, q), device_id_type=MESH)
            if start:
                pltpu.make_async_copy(rel.at[qq, b], rel.at[qq, b], rel_recv.at[qq, b]).wait()
                c.start()
            else:
                c.wait_send()

    def relay(n):
        b = lax.rem(n, bands)

        @pl.when(n // bands == lax.rem(q, per))
        def _():
            @pl.loop(0, pixes)
            def _(qq):
                pass_on(qq, b, True)

    @pl.loop(0, per * bands)
    def _(n):
        j = n // bands
        b = lax.rem(n, bands)

        @pl.when(b == 0)
        def _():
            gram_step(j)

        band_step(j, b)

        @pl.when(n >= LAG)
        def _():
            relay(n - LAG)

    part[...] = jnp.concatenate(
        [jnp.sum(ssum[b], 0, keepdims=True) for b in range(bands + 1)], 0)

    def date_part(k):
        return pltpu.make_async_remote_copy(
            part, part_date.at[s], pd_send.at[k], pd_recv.at[s],
            device_id=(lax.rem(s + k, dates), q), device_id_type=MESH)

    def pix_part(k):
        return pltpu.make_async_remote_copy(
            part_mid, part_pix.at[q], pp_send.at[k], pp_recv.at[q],
            device_id=(s, lax.rem(q + k, pixes)), device_id_type=MESH)

    for k in range(1, dates):
        date_part(k).start()
    part_date[s] = part[...]
    for n in range(LAG):
        relay(per * bands - LAG + n)
    for k in range(1, dates):
        sd = lax.rem(s + k, dates)
        pltpu.make_async_copy(part_date.at[sd], part_date.at[sd], pd_recv.at[sd]).wait()
    mid = part_date[0]
    for sd in range(1, dates):
        mid = mid + part_date[sd]
    part_mid[...] = mid
    for k in range(1, pixes):
        pix_part(k).start()
    part_pix[q] = mid

    @pl.loop(0, bands)
    def _(b):
        for c in range(per):
            pltpu.make_async_copy(fin.at[c, b], fin.at[c, b], fin_recv.at[c, b]).wait()
            for i in range(HARM):
                coef[b, i, :, c * 128:(c + 1) * 128] = fin[c, b, i]

    for k in range(1, pixes):
        qq = lax.rem(q + k, pixes)
        pltpu.make_async_copy(part_pix.at[qq], part_pix.at[qq], pp_recv.at[qq]).wait()
    tot = part_pix[0]
    for qq in range(1, pixes):
        tot = tot + part_pix[qq]
    tot = jnp.sum(tot, 1, keepdims=True)
    for b in range(bands):
        sigma = jnp.sqrt(tot[b:b + 1] / tot[bands:bands + 1])
        sigma = jnp.broadcast_to(sigma, (block, 128))
        for c in range(per):
            score[b, :, c * 128:(c + 1) * 128] = fin[c, b, HARM] / sigma

    for k in range(1, dates):
        des_copy(k).wait_send()
        date_part(k).wait_send()
    for k in range(1, pixes):
        pix_part(k).wait_send()

    @pl.loop(0, per)
    def _(j):
        for k in range(1, dates):
            code_copy(j, k).wait_send()

        @pl.loop(0, bands)
        def _(b):
            for k in range(1, dates):
                raw_copy(j, b, k).wait_send()
            hop(j, b, False)

    @pl.loop(0, pixes)
    def _(qq):
        @pl.loop(0, bands)
        def _(b):
            pass_on(qq, b, False)


def local(mesh, stack, quality, days):
    dates, pixes = mesh.shape["date"], mesh.shape["pix"]
    times, bands, rows, width = stack.shape
    block = rows // pixes
    per = pixes // dates
    total = dates * times
    des = jnp.pad(design_matrix(days), ((0, 0), (0, 128 - HARM)))
    dims = (dates, pixes, times, bands, block)
    tile = (block, width)
    vmem, dma = pltpu.VMEM, pltpu.SemaphoreType.DMA
    f32, bf16 = jnp.float32, jnp.bfloat16
    return pl.pallas_call(
        functools.partial(kernel, dims),
        out_shape=(
            jax.ShapeDtypeStruct((bands, HARM, block, width * per), f32),
            jax.ShapeDtypeStruct((bands, block, width * per), f32),
        ),
        in_specs=[
            pl.BlockSpec(memory_space=pl.ANY),
            pl.BlockSpec(memory_space=pl.ANY),
            pl.BlockSpec(memory_space=pltpu.VMEM),
        ],
        out_specs=(
            pl.BlockSpec(memory_space=pltpu.VMEM),
            pl.BlockSpec(memory_space=pltpu.VMEM),
        ),
        scratch_shapes=[
            vmem((times, rows, width), jnp.int32),
            vmem((pixes, times) + tile, bf16),
            vmem((per, bands + 1, total) + tile, bf16),
            vmem((dates, times, 128), f32),
            vmem((total, HARM) + tile, f32),
            vmem((total,) + tile, f32),
            vmem((len(PAIR_LIST),) + tile, f32),
            vmem(tile, f32),
            vmem((per, bands, HARM + 1) + tile, f32),
            vmem((pixes, bands, HARM + 1) + tile, f32),
            vmem((per, bands, HARM + 1) + tile, f32),
            vmem((bands + 1,) + tile, f32),
            vmem((bands + 1, width), f32),
            vmem((dates, bands + 1, width), f32),
            vmem((bands + 1, width), f32),
            vmem((pixes, bands + 1, width), f32),
            dma,
            dma((dates,)),
            dma((dates,)),
            dma((per, bands + 1, dates)),
            dma((per, bands + 1, dates)),
            dma((per, bands)),
            dma((pixes, bands)),
            dma((pixes, bands)),
            dma((per, bands)),
            dma((dates,)),
            dma((dates,)),
            dma((pixes,)),
            dma((pixes,)),
        ],
        compiler_params=pltpu.CompilerParams(
            collective_id=0, has_side_effects=True, vmem_limit_bytes=60000000
        ),
    )(stack, quality, des)


def solution(mesh):
    return jax.shard_map(
        functools.partial(local, mesh),
        mesh=mesh,
        in_specs=(P("date", None, None, "pix"), P("date", None, "pix"), P("date")),
        out_specs=(P(None, None, "pix", "date"), P(None, "pix", "date")),
        check_vma=False,
    )
```

```python
import functools

import jax
import jax.numpy as jnp
from jax import lax
from jax.experimental import pallas as pl
from jax.experimental.pallas import tpu as pltpu
from jax.sharding import PartitionSpec as P

RIDGE_TERM = 1.0
HARM = 8
LAG = 2
MESH = pl.DeviceIdType.MESH
PAIR_LIST = [(first, second) for first in range(HARM) for second in range(first + 1)]
PAIR_AT = {pair: number for number, pair in enumerate(PAIR_LIST)}


def design_lanes(days):
    rows = [jnp.full((1, 128), day, jnp.int32) for day in days]
    moment_t = jnp.concatenate(rows, 0).astype(jnp.float32)
    lane = lax.broadcasted_iota(jnp.int32, moment_t.shape, 1)
    rate = jnp.where(
        lane < 4, 2.0 * jnp.pi, jnp.where(lane < 6, 4.0 * jnp.pi, 6.0 * jnp.pi))
    phase = rate * moment_t / 365.25
    wave = jnp.where(jnp.bitwise_and(lane, 1) == 0, jnp.cos(phase), jnp.sin(phase))
    linear = (moment_t - 512.0) / 512.0
    return jnp.where(lane == 0, 1.0, jnp.where(lane == 1, linear, wave))


def kernel(dims, stack, quality, days, fin, tot_ref,
           des_in, qbuf, code, raw, dall, bdes, wbuf, lbuf, wsum_ref, res, rel,
           ssum, part, part_date, part_mid, part_pix,
           q_sem, des_send, des_recv, raw_send, raw_recv,
           hop_send, rel_recv, fin_send, fin_recv,
           pd_send, pd_recv, pp_send, pp_recv):
    dates, pixes, times, bands, block = dims
    per = pixes // dates
    s = lax.axis_index("date")
    q = lax.axis_index("pix")
    total = dates * times

    def peer_of(k):
        if dates & (dates - 1):
            return lax.rem(s + k, dates)
        return jnp.bitwise_xor(s, k)

    home = q // per

    def target(sd, j):
        return per * lax.rem(sd + per * lax.rem(q, 2) + j, dates) + j

    def owner(qq, p):
        shift = per * lax.rem(qq, 2) + lax.rem(p, per)
        return lax.rem(p // per + 64 * dates - shift, dates)

    barrier = pltpu.get_barrier_semaphore()
    for k in range(1, dates):
        pl.semaphore_signal(barrier, inc=1, device_id=(peer_of(k), q),
                            device_id_type=MESH)
    for k in range(1, pixes):
        pl.semaphore_signal(barrier, inc=1, device_id=(s, lax.rem(q + k, pixes)),
                            device_id_type=MESH)

    q_copy = pltpu.make_async_copy(quality, qbuf, q_sem)
    q_copy.start()

    def own_copy(j, b):
        rows = pl.ds(pl.multiple_of(target(s, j) * block, block), block)
        return pltpu.make_async_copy(
            stack.at[:, b, rows, :], raw.at[j, b, pl.ds(s * times, times)],
            raw_recv.at[j, b, s])

    def own_code(j):
        return pltpu.make_async_copy(
            code.at[target(s, j)], raw.at[j, bands, pl.ds(s * times, times)],
            raw_recv.at[j, bands, s])

    for j in range(per):
        for b in range(bands):
            own_copy(j, b).start()

    des_in[...] = design_lanes([days[r] for r in range(times)])
    q_copy.wait()
    for p in range(pixes):
        bits = qbuf[:, p * block:(p + 1) * block, :]
        cloud = jnp.bitwise_and(jnp.right_shift(bits, 3), 1)
        level = jnp.bitwise_and(jnp.right_shift(bits, 8), 3)
        code[p] = ((1 - cloud) * (1 + level)).astype(jnp.float32).astype(jnp.bfloat16)

    pl.semaphore_wait(barrier, dates - 1 + pixes - 1)

    def des_copy(k):
        return pltpu.make_async_remote_copy(
            des_in, dall.at[s], des_send.at[k], des_recv.at[s],
            device_id=(peer_of(k), q), device_id_type=MESH)

    def raw_copy(j, b, k):
        peer = peer_of(k)
        rows = pl.ds(pl.multiple_of(target(peer, j) * block, block), block)
        return pltpu.make_async_remote_copy(
            stack.at[:, b, rows, :], raw.at[j, b, pl.ds(s * times, times)],
            raw_send.at[j, b, k], raw_recv.at[j, b, s],
            device_id=(peer, q), device_id_type=MESH)

    def code_copy(j, k):
        peer = peer_of(k)
        return pltpu.make_async_remote_copy(
            code.at[target(peer, j)], raw.at[j, bands, pl.ds(s * times, times)],
            raw_send.at[j, bands, k], raw_recv.at[j, bands, s],
            device_id=(peer, q), device_id_type=MESH)

    for k in range(1, dates):
        des_copy(k).start()
    for j in range(per):
        own_code(j).start()
        for k in range(1, dates):
            code_copy(j, k).start()
    for j in range(per):
        for b in range(bands):
            for k in range(1, dates):
                raw_copy(j, b, k).start()

    def raw_wait(j, b, sd):
        pltpu.make_async_copy(
            raw.at[j, b, pl.ds(sd * times, times)],
            raw.at[j, b, pl.ds(sd * times, times)],
            raw_recv.at[j, b, sd]).wait()

    dall[s] = des_in[...]
    for k in range(1, dates):
        sd = peer_of(k)
        pltpu.make_async_copy(dall.at[sd], dall.at[sd], des_recv.at[sd]).wait()

    @pl.loop(0, total, unroll=4)
    def _(t):
        row = dall[t // times, pl.ds(lax.rem(t, times), 1), :]
        for i in range(HARM):
            bdes[t, i] = jnp.broadcast_to(row[:, i:i + 1], (block, 128))

    zero = jnp.zeros((block, 128), jnp.float32)
    for b in range(bands + 1):
        ssum[b] = zero

    def gram_step(j):
        for sd in range(dates):
            raw_wait(j, bands, sd)

        def body(t, carry):
            value = raw[j, bands, t].astype(jnp.float32)
            w = jnp.where(value == 0.0, 0.0, 1.0 / jnp.maximum(value, 1.0))
            wbuf[t] = w
            d = [bdes[t, i] for i in range(HARM)]
            wd = [w] + [w * d[i] for i in range(1, HARM)]
            return tuple(
                carry[n] + (wd[first] if second == 0 else wd[first] * d[second])
                for n, (first, second) in enumerate(PAIR_LIST))

        gram = lax.fori_loop(0, total, body, (zero,) * len(PAIR_LIST), unroll=2)
        wsum_ref[...] = gram[0]
        ssum[bands] = ssum[bands] + gram[0]
        lower = {}
        for first in range(HARM):
            for second in range(first + 1):
                value = gram[PAIR_AT[first, second]]
                if first == second:
                    value = value + RIDGE_TERM
                for inner in range(second):
                    value = value - lower[first, inner] * lower[second, inner]
                if first == second:
                    lower[first, first] = 1.0 / jnp.sqrt(value)
                else:
                    lower[first, second] = value * lower[second, second]
                lbuf[PAIR_AT[first, second]] = lower[first, second]

    def hop(j, b, start):
        p = target(s, j)

        def act(dst, sem):
            @pl.when(p != q)
            def _():
                c = pltpu.make_async_remote_copy(
                    res.at[j, b], dst, hop_send.at[j, b], sem,
                    device_id=(s, p), device_id_type=MESH)
                c.start() if start else c.wait_send()

            if start:
                @pl.when(p == q)
                def _():
                    pltpu.make_async_copy(res.at[j, b], dst, sem).start()

        @pl.when(home == s)
        def _():
            act(fin.at[lax.rem(q, per), b], fin_recv.at[lax.rem(q, per), b])

        @pl.when(home != s)
        def _():
            act(rel.at[q, b], rel_recv.at[q, b])

    def band_step(j, b):
        for sd in range(dates):
            raw_wait(j, b, sd)

        def body(t, carry):
            wy = wbuf[t] * raw[j, b, t].astype(jnp.float32)
            return tuple(
                carry[i] + (wy if i == 0 else bdes[t, i] * wy) for i in range(HARM))

        moment = lax.fori_loop(0, total, body, (zero,) * HARM, unroll=8)
        low = lambda first, second: lbuf[PAIR_AT[first, second]]
        forward = []
        for first in range(HARM):
            value = moment[first]
            for inner in range(first):
                value = value - low(first, inner) * forward[inner]
            forward.append(value * low(first, first))
        back = [None] * HARM
        for first in range(HARM - 1, -1, -1):
            value = forward[first]
            for inner in range(HARM - 1, first, -1):
                value = value - low(inner, first) * back[inner]
            back[first] = value * low(first, first)
        for i in range(HARM):
            res[j, b, i] = back[i]

        def residual(t, ssr):
            terms = [back[0]] + [bdes[t, i] * back[i] for i in range(1, HARM)]
            while len(terms) > 1:
                terms = [terms[i] + terms[i + 1] for i in range(0, len(terms), 2)]
            diff = raw[j, b, t].astype(jnp.float32) - terms[0]
            return ssr + wbuf[t] * diff * diff

        ssr = lax.fori_loop(0, total, residual, zero, unroll=8)
        res[j, b, HARM] = jnp.sqrt(ssr / (wsum_ref[...] + 1.0))
        ssum[b] = ssum[b] + ssr
        hop(j, b, True)

    def pass_on(qq, b, start):
        far = qq // per

        @pl.when(jnp.logical_and(owner(qq, q) == s, far != s))
        def _():
            c = pltpu.make_async_remote_copy(
                rel.at[qq, b], fin.at[lax.rem(qq, per), b], fin_send.at[qq, b],
                fin_recv.at[lax.rem(qq, per), b],
                device_id=(far, q), device_id_type=MESH)
            if start:
                pltpu.make_async_copy(rel.at[qq, b], rel.at[qq, b], rel_recv.at[qq, b]).wait()
                c.start()
            else:
                c.wait_send()

    def relay(n):
        b = lax.rem(n, bands)

        @pl.when(n // bands == lax.rem(q, per))
        def _():
            @pl.loop(0, pixes)
            def _(qq):
                pass_on(qq, b, True)

    @pl.loop(0, per * bands)
    def _(n):
        j = n // bands
        b = lax.rem(n, bands)

        @pl.when(b == 0)
        def _():
            gram_step(j)

        band_step(j, b)

        @pl.when(n >= LAG)
        def _():
            relay(n - LAG)

    part[...] = jnp.concatenate(
        [jnp.sum(ssum[b], 0, keepdims=True) for b in range(bands + 1)], 0)

    def date_part(k):
        return pltpu.make_async_remote_copy(
            part, part_date.at[s], pd_send.at[k], pd_recv.at[s],
            device_id=(peer_of(k), q), device_id_type=MESH)

    def pix_part(k):
        return pltpu.make_async_remote_copy(
            part_mid, part_pix.at[q], pp_send.at[k], pp_recv.at[q],
            device_id=(s, lax.rem(q + k, pixes)), device_id_type=MESH)

    for k in range(1, dates):
        date_part(k).start()
    part_date[s] = part[...]
    for n in range(LAG):
        relay(per * bands - LAG + n)
    for k in range(1, dates):
        sd = peer_of(k)
        pltpu.make_async_copy(part_date.at[sd], part_date.at[sd], pd_recv.at[sd]).wait()
    mid = part_date[0]
    for sd in range(1, dates):
        mid = mid + part_date[sd]
    part_mid[...] = mid
    for k in range(1, pixes):
        pix_part(k).start()
    part_pix[q] = mid

    @pl.loop(0, bands)
    def _(b):
        for c in range(per):
            pltpu.make_async_copy(fin.at[c, b], fin.at[c, b], fin_recv.at[c, b]).wait()

    for k in range(1, pixes):
        qq = lax.rem(q + k, pixes)
        pltpu.make_async_copy(part_pix.at[qq], part_pix.at[qq], pp_recv.at[qq]).wait()
    tot = part_pix[0]
    for qq in range(1, pixes):
        tot = tot + part_pix[qq]
    tot_ref[...] = tot

    for k in range(1, dates):
        des_copy(k).wait_send()
        date_part(k).wait_send()
    for k in range(1, pixes):
        pix_part(k).wait_send()

    @pl.loop(0, per)
    def _(j):
        for k in range(1, dates):
            code_copy(j, k).wait_send()

        @pl.loop(0, bands)
        def _(b):
            for k in range(1, dates):
                raw_copy(j, b, k).wait_send()
            hop(j, b, False)

    @pl.loop(0, pixes)
    def _(qq):
        @pl.loop(0, bands)
        def _(b):
            pass_on(qq, b, False)


def finish(fin, tot_ref, coef, score):
    per, bands = fin.shape[:2]
    tot = jnp.sum(tot_ref[...], 1, keepdims=True)
    for b in range(bands):
        sigma = jnp.sqrt(tot[b:b + 1] / tot[bands:bands + 1])
        scale = jnp.broadcast_to(1.0 / sigma, fin.shape[3:])
        for c in range(per):
            cols = slice(c * 128, (c + 1) * 128)
            for i in range(HARM):
                coef[b, i, :, cols] = fin[c, b, i]
            score[b, :, cols] = fin[c, b, HARM] * scale


def local(mesh, stack, quality, days):
    dates, pixes = mesh.shape["date"], mesh.shape["pix"]
    times, bands, rows, width = stack.shape
    block = rows // pixes
    per = pixes // dates
    total = dates * times
    dims = (dates, pixes, times, bands, block)
    tile = (block, width)
    vmem, dma = pltpu.VMEM, pltpu.SemaphoreType.DMA
    f32, bf16 = jnp.float32, jnp.bfloat16
    fin, tot = pl.pallas_call(
        functools.partial(kernel, dims),
        out_shape=(
            jax.ShapeDtypeStruct((per, bands, HARM + 1) + tile, f32),
            jax.ShapeDtypeStruct((bands + 1, width), f32),
        ),
        in_specs=[
            pl.BlockSpec(memory_space=pl.ANY),
            pl.BlockSpec(memory_space=pl.ANY),
            pl.BlockSpec(memory_space=pltpu.SMEM),
        ],
        out_specs=(
            pl.BlockSpec(memory_space=pl.ANY),
            pl.BlockSpec(memory_space=pltpu.VMEM),
        ),
        scratch_shapes=[
            vmem((times, 128), f32),
            vmem((times, rows, width), jnp.int32),
            vmem((pixes, times) + tile, bf16),
            vmem((per, bands + 1, total) + tile, bf16),
            vmem((dates, times, 128), f32),
            vmem((total, HARM) + tile, f32),
            vmem((total,) + tile, f32),
            vmem((len(PAIR_LIST),) + tile, f32),
            vmem(tile, f32),
            vmem((per, bands, HARM + 1) + tile, f32),
            vmem((pixes, bands, HARM + 1) + tile, f32),
            vmem((bands + 1,) + tile, f32),
            vmem((bands + 1, width), f32),
            vmem((dates, bands + 1, width), f32),
            vmem((bands + 1, width), f32),
            vmem((pixes, bands + 1, width), f32),
            dma,
            dma((dates,)),
            dma((dates,)),
            dma((per, bands + 1, dates)),
            dma((per, bands + 1, dates)),
            dma((per, bands)),
            dma((pixes, bands)),
            dma((pixes, bands)),
            dma((per, bands)),
            dma((dates,)),
            dma((dates,)),
            dma((pixes,)),
            dma((pixes,)),
        ],
        compiler_params=pltpu.CompilerParams(
            collective_id=0, has_side_effects=True, vmem_limit_bytes=60000000
        ),
    )(stack, quality, days)
    whole = pl.BlockSpec(memory_space=pltpu.VMEM)
    return pl.pallas_call(
        finish,
        out_shape=(
            jax.ShapeDtypeStruct((bands, HARM, block, width * per), f32),
            jax.ShapeDtypeStruct((bands, block, width * per), f32),
        ),
        in_specs=[whole, whole],
        out_specs=(whole, whole),
    )(fin, tot)


def solution(mesh):
    return jax.shard_map(
        functools.partial(local, mesh),
        mesh=mesh,
        in_specs=(P("date", None, None, "pix"), P("date", None, "pix"), P("date")),
        out_specs=(P(None, None, "pix", "date"), P(None, "pix", "date")),
        check_vma=False,
    )
```

```python
import functools

import jax
import jax.numpy as jnp
from jax import lax
from jax.experimental import pallas as pl
from jax.experimental.pallas import tpu as pltpu
from jax.sharding import PartitionSpec as P

RIDGE_TERM = 1.0
HARM = 8
LAG = 4
EARLY = 1
LIMIT = 32767.0


def ORDER(dates):
    return range(dates - 1, 0, -1)
MESH = pl.DeviceIdType.MESH
PAIR_LIST = [(first, second) for first in range(HARM) for second in range(first + 1)]
PAIR_AT = {pair: number for number, pair in enumerate(PAIR_LIST)}


def design_lanes(days):
    rows = [jnp.full((1, 128), day, jnp.int32) for day in days]
    moment_t = jnp.concatenate(rows, 0).astype(jnp.float32)
    lane = lax.broadcasted_iota(jnp.int32, moment_t.shape, 1)
    rate = jnp.where(
        lane < 4, 2.0 * jnp.pi, jnp.where(lane < 6, 4.0 * jnp.pi, 6.0 * jnp.pi))
    phase = rate * moment_t / 365.25
    wave = jnp.where(jnp.bitwise_and(lane, 1) == 0, jnp.cos(phase), jnp.sin(phase))
    linear = (moment_t - 512.0) / 512.0
    return jnp.where(lane == 0, 1.0, jnp.where(lane == 1, linear, wave))


def kernel(dims, stack, quality, days, fin, tot_ref,
           des_in, qbuf, code, raw, dall, bdes, wbuf, lbuf, wsum_ref, res, rel,
           ssum, part, part_date, part_mid, part_pix,
           q_sem, des_send, des_recv, raw_send, raw_recv,
           hop_send, rel_recv, fin_send, fin_recv,
           pd_send, pd_recv, pp_send, pp_recv):
    dates, pixes, times, bands, block = dims
    per = pixes // dates
    s = lax.axis_index("date")
    q = lax.axis_index("pix")
    total = dates * times

    def peer_of(k):
        if dates & (dates - 1):
            return lax.rem(s + k, dates)
        return jnp.bitwise_xor(s, k)

    home = q // per

    def target(sd, j):
        return per * lax.rem(sd + per * lax.rem(q, 2) + j, dates) + j

    def owner(qq, p):
        shift = per * lax.rem(qq, 2) + lax.rem(p, per)
        return lax.rem(p // per + 64 * dates - shift, dates)

    barrier = pltpu.get_barrier_semaphore()
    for k in range(1, dates):
        pl.semaphore_signal(barrier, inc=1, device_id=(peer_of(k), q),
                            device_id_type=MESH)
    for k in range(1, pixes):
        pl.semaphore_signal(barrier, inc=1, device_id=(s, lax.rem(q + k, pixes)),
                            device_id_type=MESH)

    q_copy = pltpu.make_async_copy(quality, qbuf, q_sem)
    q_copy.start()

    def own_copy(j, b):
        rows = pl.ds(pl.multiple_of(target(s, j) * block, block), block)
        return pltpu.make_async_copy(
            stack.at[:, b, rows, :], raw.at[j, b, pl.ds(s * times, times)],
            raw_recv.at[j, b, s])

    def own_code(j):
        return pltpu.make_async_copy(
            code.at[target(s, j)], raw.at[j, bands, pl.ds(s * times, times)],
            raw_recv.at[j, bands, s])

    for j in range(per):
        for b in range(bands):
            own_copy(j, b).start()

    pl.semaphore_wait(barrier, dates - 1 + pixes - 1)

    def des_copy(k):
        return pltpu.make_async_remote_copy(
            des_in, dall.at[s], des_send.at[k], des_recv.at[s],
            device_id=(peer_of(k), q), device_id_type=MESH)

    def raw_copy(j, b, k):
        peer = peer_of(k)
        rows = pl.ds(pl.multiple_of(target(peer, j) * block, block), block)
        return pltpu.make_async_remote_copy(
            stack.at[:, b, rows, :], raw.at[j, b, pl.ds(s * times, times)],
            raw_send.at[j, b, k], raw_recv.at[j, b, s],
            device_id=(peer, q), device_id_type=MESH)

    def code_copy(j, k):
        peer = peer_of(k)
        return pltpu.make_async_remote_copy(
            code.at[target(peer, j)], raw.at[j, bands, pl.ds(s * times, times)],
            raw_send.at[j, bands, k], raw_recv.at[j, bands, s],
            device_id=(peer, q), device_id_type=MESH)

    for b in range(EARLY):
        for k in ORDER(dates):
            raw_copy(0, b, k).start()

    des_in[...] = design_lanes([days[r] for r in range(times)])
    q_copy.wait()
    for p in range(pixes):
        bits = qbuf[:, p * block:(p + 1) * block, :]
        cloud = jnp.bitwise_and(jnp.right_shift(bits, 3), 1)
        level = jnp.bitwise_and(jnp.right_shift(bits, 8), 3)
        code[p] = ((1 - cloud) * (1 + level)).astype(jnp.float32).astype(jnp.bfloat16)

    for k in range(1, dates):
        des_copy(k).start()
    for j in range(per):
        own_code(j).start()
        for k in range(1, dates):
            code_copy(j, k).start()
    for j in range(per):
        for b in range(EARLY if j == 0 else 0, bands):
            for k in ORDER(dates):
                raw_copy(j, b, k).start()

    def raw_wait(j, b, sd):
        pltpu.make_async_copy(
            raw.at[j, b, pl.ds(sd * times, times)],
            raw.at[j, b, pl.ds(sd * times, times)],
            raw_recv.at[j, b, sd]).wait()

    dall[s] = des_in[...]
    for k in range(1, dates):
        sd = peer_of(k)
        pltpu.make_async_copy(dall.at[sd], dall.at[sd], des_recv.at[sd]).wait()

    @pl.loop(0, total, unroll=4)
    def _(t):
        row = dall[t // times, pl.ds(lax.rem(t, times), 1), :]
        for i in range(HARM):
            bdes[t, i] = jnp.broadcast_to(row[:, i:i + 1], (block, 128))

    zero = jnp.zeros((block, 128), jnp.float32)
    for b in range(bands + 1):
        ssum[b] = zero

    def gram_step(j):
        for sd in range(dates):
            raw_wait(j, bands, sd)

        def body(t, carry):
            value = raw[j, bands, t].astype(jnp.float32)
            w = jnp.where(value == 0.0, 0.0, 1.0 / jnp.maximum(value, 1.0))
            wbuf[t] = w
            d = [bdes[t, i] for i in range(HARM)]
            wd = [w] + [w * d[i] for i in range(1, HARM)]
            return tuple(
                carry[n] + (wd[first] if second == 0 else wd[first] * d[second])
                for n, (first, second) in enumerate(PAIR_LIST))

        gram = lax.fori_loop(0, total, body, (zero,) * len(PAIR_LIST), unroll=2)
        wsum_ref[...] = gram[0]
        ssum[bands] = ssum[bands] + gram[0]
        lower = {}
        for first in range(HARM):
            for second in range(first + 1):
                value = gram[PAIR_AT[first, second]]
                if first == second:
                    value = value + RIDGE_TERM
                for inner in range(second):
                    value = value - lower[first, inner] * lower[second, inner]
                if first == second:
                    lower[first, first] = 1.0 / jnp.sqrt(value)
                else:
                    lower[first, second] = value * lower[second, second]
                lbuf[PAIR_AT[first, second]] = lower[first, second]

    def hop(j, b, start):
        p = target(s, j)

        def act(dst, sem):
            @pl.when(p != q)
            def _():
                c = pltpu.make_async_remote_copy(
                    res.at[j, b], dst, hop_send.at[j, b], sem,
                    device_id=(s, p), device_id_type=MESH)
                c.start() if start else c.wait_send()

            if start:
                @pl.when(p == q)
                def _():
                    pltpu.make_async_copy(res.at[j, b], dst, sem).start()

        @pl.when(home == s)
        def _():
            act(fin.at[lax.rem(q, per), b], fin_recv.at[lax.rem(q, per), b])

        @pl.when(home != s)
        def _():
            act(rel.at[q, b], rel_recv.at[q, b])

    def band_step(j, b):
        for sd in range(dates):
            raw_wait(j, b, sd)

        def body(t, carry):
            wy = wbuf[t] * raw[j, b, t].astype(jnp.float32)
            return tuple(
                carry[i] + (wy if i == 0 else bdes[t, i] * wy) for i in range(HARM))

        moment = lax.fori_loop(0, total, body, (zero,) * HARM, unroll=8)
        low = lambda first, second: lbuf[PAIR_AT[first, second]]
        forward = []
        for first in range(HARM):
            value = moment[first]
            for inner in range(first):
                value = value - low(first, inner) * forward[inner]
            forward.append(value * low(first, first))
        back = [None] * HARM
        for first in range(HARM - 1, -1, -1):
            value = forward[first]
            for inner in range(HARM - 1, first, -1):
                value = value - low(inner, first) * back[inner]
            back[first] = value * low(first, first)
        peak = jnp.abs(back[0])
        for i in range(1, HARM):
            peak = jnp.maximum(peak, jnp.abs(back[i]))
        level = power(peak)
        inverse = jnp.exp2(-level)
        for i in range(HARM):
            res[j, b, i] = encode(back[i], inverse)

        def residual(t, ssr):
            terms = [back[0]] + [bdes[t, i] * back[i] for i in range(1, HARM)]
            while len(terms) > 1:
                terms = [terms[i] + terms[i + 1] for i in range(0, len(terms), 2)]
            diff = raw[j, b, t].astype(jnp.float32) - terms[0]
            return ssr + wbuf[t] * diff * diff

        ssr = lax.fori_loop(0, total, residual, zero, unroll=8)
        ratio = jnp.sqrt(ssr / (wsum_ref[...] + 1.0))
        ratio_level = power(ratio)
        res[j, b, HARM] = encode(ratio, jnp.exp2(-ratio_level))
        lane = lax.broadcasted_iota(jnp.int32, ratio.shape, 1)
        both = jnp.where(lane == 0, level, ratio_level)
        res[j, b, HARM + 1] = both.astype(jnp.int32).astype(jnp.int16)
        ssum[b] = ssum[b] + ssr
        hop(j, b, True)

    def pass_on(qq, b, start):
        far = qq // per

        @pl.when(jnp.logical_and(owner(qq, q) == s, far != s))
        def _():
            c = pltpu.make_async_remote_copy(
                rel.at[qq, b], fin.at[lax.rem(qq, per), b], fin_send.at[qq, b],
                fin_recv.at[lax.rem(qq, per), b],
                device_id=(far, q), device_id_type=MESH)
            if start:
                pltpu.make_async_copy(rel.at[qq, b], rel.at[qq, b], rel_recv.at[qq, b]).wait()
                c.start()
            else:
                c.wait_send()

    def relay(n):
        b = lax.rem(n, bands)

        @pl.when(n // bands == lax.rem(q, per))
        def _():
            @pl.loop(0, pixes)
            def _(qq):
                pass_on(qq, b, True)

    @pl.loop(0, per * bands)
    def _(n):
        j = n // bands
        b = lax.rem(n, bands)

        @pl.when(b == 0)
        def _():
            gram_step(j)

        band_step(j, b)

        @pl.when(n >= LAG)
        def _():
            relay(n - LAG)

    part[...] = jnp.concatenate(
        [jnp.sum(ssum[b], 0, keepdims=True) for b in range(bands + 1)], 0)

    def date_part(k):
        return pltpu.make_async_remote_copy(
            part, part_date.at[s], pd_send.at[k], pd_recv.at[s],
            device_id=(peer_of(k), q), device_id_type=MESH)

    def pix_part(k):
        return pltpu.make_async_remote_copy(
            part_mid, part_pix.at[q], pp_send.at[k], pp_recv.at[q],
            device_id=(s, lax.rem(q + k, pixes)), device_id_type=MESH)

    for k in range(1, dates):
        date_part(k).start()
    part_date[s] = part[...]
    for n in range(LAG):
        relay(per * bands - LAG + n)
    for k in range(1, dates):
        sd = peer_of(k)
        pltpu.make_async_copy(part_date.at[sd], part_date.at[sd], pd_recv.at[sd]).wait()
    mid = part_date[0]
    for sd in range(1, dates):
        mid = mid + part_date[sd]
    part_mid[...] = mid
    for k in range(1, pixes):
        pix_part(k).start()
    part_pix[q] = mid

    @pl.loop(0, bands)
    def _(b):
        for c in range(per):
            pltpu.make_async_copy(fin.at[c, b], fin.at[c, b], fin_recv.at[c, b]).wait()

    for k in range(1, pixes):
        qq = lax.rem(q + k, pixes)
        pltpu.make_async_copy(part_pix.at[qq], part_pix.at[qq], pp_recv.at[qq]).wait()
    tot = part_pix[0]
    for qq in range(1, pixes):
        tot = tot + part_pix[qq]
    tot_ref[...] = tot

    for k in range(1, dates):
        des_copy(k).wait_send()
        date_part(k).wait_send()
    for k in range(1, pixes):
        pix_part(k).wait_send()

    @pl.loop(0, per)
    def _(j):
        for k in range(1, dates):
            code_copy(j, k).wait_send()

        @pl.loop(0, bands)
        def _(b):
            for k in range(1, dates):
                raw_copy(j, b, k).wait_send()
            hop(j, b, False)

    @pl.loop(0, pixes)
    def _(qq):
        @pl.loop(0, bands)
        def _(b):
            pass_on(qq, b, False)


def power(value):
    peak = jnp.max(jnp.max(value, 0, keepdims=True), 1, keepdims=True)
    level = jnp.ceil(jnp.log2(jnp.maximum(peak, 1e-36)) + 0.01)
    return jnp.broadcast_to(level, value.shape)


def encode(value, inverse):
    root = jnp.sqrt(jnp.minimum(jnp.abs(value) * inverse, 1.0)) * LIMIT + 0.5
    root = jnp.floor(root)
    return jnp.where(value < 0.0, -root, root).astype(jnp.int32).astype(jnp.int16)


def decode(value, scale):
    root = value.astype(jnp.int32).astype(jnp.float32) * (1.0 / LIMIT)
    return root * jnp.abs(root) * scale


def finish(fin, tot_ref, coef, score):
    per, bands = fin.shape[:2]
    tot = jnp.sum(tot_ref[...], 1, keepdims=True)
    for b in range(bands):
        sigma = jnp.sqrt(tot[b:b + 1] / tot[bands:bands + 1])
        scale = jnp.broadcast_to(1.0 / sigma, fin.shape[3:])
        for c in range(per):
            cols = slice(c * 128, (c + 1) * 128)
            both = fin[c, b, HARM + 1].astype(jnp.int32).astype(jnp.float32)
            unit = jnp.broadcast_to(jnp.exp2(both[:, 0:1]), both.shape)
            ratio_unit = jnp.broadcast_to(jnp.exp2(both[:, 1:2]), both.shape)
            for i in range(HARM):
                coef[b, i, :, cols] = decode(fin[c, b, i], unit)
            score[b, :, cols] = decode(fin[c, b, HARM], ratio_unit) * scale


def local(mesh, stack, quality, days):
    dates, pixes = mesh.shape["date"], mesh.shape["pix"]
    times, bands, rows, width = stack.shape
    block = rows // pixes
    per = pixes // dates
    total = dates * times
    dims = (dates, pixes, times, bands, block)
    tile = (block, width)
    vmem, dma = pltpu.VMEM, pltpu.SemaphoreType.DMA
    f32, bf16 = jnp.float32, jnp.bfloat16
    fin, tot = pl.pallas_call(
        functools.partial(kernel, dims),
        out_shape=(
            jax.ShapeDtypeStruct((per, bands, HARM + 2) + tile, jnp.int16),
            jax.ShapeDtypeStruct((bands + 1, width), f32),
        ),
        in_specs=[
            pl.BlockSpec(memory_space=pl.ANY),
            pl.BlockSpec(memory_space=pl.ANY),
            pl.BlockSpec(memory_space=pltpu.SMEM),
        ],
        out_specs=(
            pl.BlockSpec(memory_space=pl.ANY),
            pl.BlockSpec(memory_space=pltpu.VMEM),
        ),
        scratch_shapes=[
            vmem((times, 128), f32),
            vmem((times, rows, width), jnp.int32),
            vmem((pixes, times) + tile, bf16),
            vmem((per, bands + 1, total) + tile, bf16),
            vmem((dates, times, 128), f32),
            vmem((total, HARM) + tile, f32),
            vmem((total,) + tile, f32),
            vmem((len(PAIR_LIST),) + tile, f32),
            vmem(tile, f32),
            vmem((per, bands, HARM + 2) + tile, jnp.int16),
            vmem((pixes, bands, HARM + 2) + tile, jnp.int16),
            vmem((bands + 1,) + tile, f32),
            vmem((bands + 1, width), f32),
            vmem((dates, bands + 1, width), f32),
            vmem((bands + 1, width), f32),
            vmem((pixes, bands + 1, width), f32),
            dma,
            dma((dates,)),
            dma((dates,)),
            dma((per, bands + 1, dates)),
            dma((per, bands + 1, dates)),
            dma((per, bands)),
            dma((pixes, bands)),
            dma((pixes, bands)),
            dma((per, bands)),
            dma((dates,)),
            dma((dates,)),
            dma((pixes,)),
            dma((pixes,)),
        ],
        compiler_params=pltpu.CompilerParams(
            collective_id=0, has_side_effects=True, vmem_limit_bytes=60000000
        ),
    )(stack, quality, days)
    whole = pl.BlockSpec(memory_space=pltpu.VMEM)
    return pl.pallas_call(
        finish,
        out_shape=(
            jax.ShapeDtypeStruct((bands, HARM, block, width * per), f32),
            jax.ShapeDtypeStruct((bands, block, width * per), f32),
        ),
        in_specs=[whole, whole],
        out_specs=(whole, whole),
    )(fin, tot)


def solution(mesh):
    return jax.shard_map(
        functools.partial(local, mesh),
        mesh=mesh,
        in_specs=(P("date", None, None, "pix"), P("date", None, "pix"), P("date")),
        out_specs=(P(None, None, "pix", "date"), P(None, "pix", "date")),
        check_vma=False,
    )
```
